32 devices in a mesh: blk: 8 (over z, y), grp: 4 (over x, core).
Axes of the slice: x: 2, y: 2, z: 4, core: 2. Of those that a mesh axis runs over, the one named last changes fastest.
Arguments:
- frames: bfloat16 [4, 2048, 1024], P('grp', 'blk'), may hold values from -16 to 16
- utt_lengths: int32 [4], replicated, may hold values from 1 to 4096, 8192 in all
- attn_gain: float32 [1024], replicated, may hold values from 0.25 to 1.75
- w_qkv: bfloat16 [1024, 3072], P(None, 'grp'), may hold values from -4 to 4
- w_out: bfloat16 [1024, 1024], replicated, may hold values from -0.375 to 0.375
- conv_gain: float32 [1024], replicated, may hold values from 0.25 to 1.75
- w_glu: bfloat16 [1024, 2048], replicated, may hold values from -0.1875 to 0.1875
- w_depth: float32 [31, 1024], replicated, may hold values from -1 to 1
- depth_gain: float32 [1024], replicated, may hold values from 0.25 to 1.75
- w_proj: bfloat16 [1024, 1024], replicated, may hold values from -0.1875 to 0.1875
Outputs:
- block_out: bfloat16 [4, 2048, 1024], P('grp', 'blk')
The draws below stay inside these ranges and needn't reach their ends.
Inputs may be any that keep to these rules, and one draw needn't show every extreme that they name: `utt_lengths`: they sum to 8192 and the longest is exactly 4096.
All inputs are finite; a program needn't handle non-finite values.
Results may differ from the reference program's by a relative error of at most 0.0095.
Values may be sent and summed in bfloat16 or wider, within the bound.
No kernel may reach another device: no remote copies, remote signals or barrier semaphores. Data moves between devices by JAX's collectives and lax.ppermute only.
A program may use at most 192 MiB of HBM per device.

```python
import math
import jax
import jax.numpy as jnp
import numpy as np
from jax import lax

D = 1024
HEADS = 16
KERNEL = 31
WINDOW = 2048
GROUPS = 4
TOKENS = 8192
UTT_MOST = 4096
UTTERANCES = 4


def draw_frames(key, part):
    base_key = jax.random.fold_in(jax.random.fold_in(key, 11), 0)
    drawn = jax.random.normal(base_key, (GROUPS, WINDOW, D), jnp.float32)
    return jnp.clip(drawn, -16.0, 16.0).astype(jnp.bfloat16)


def draw_w_qkv(key, part):
    drawn = jax.random.normal(jax.random.fold_in(key, 23), (D, HEADS, 3, D // HEADS), jnp.float32) * (1.4 / math.sqrt(D))
    return jnp.clip(drawn.reshape(D, 3 * D), -4.0, 4.0).astype(jnp.bfloat16)


def length_profile(amount, total, most, slope):
    loads = [(1 << 20) // math.isqrt(grade ** slope) + 1 for grade in range(2, amount + 1)]
    surplus, counts = total - most - (amount - 1), [1] * (amount - 1)
    while surplus > 0:
        candidates = [i for i in range(amount - 1) if counts[i] < most]
        pool, remaining = sum([loads[i] for i in candidates]), surplus
        for i in candidates:
            addition = min(most - counts[i], max(1, remaining * loads[i] // pool), surplus)
            counts[i] = counts[i] + addition
            surplus = surplus - addition
    return np.array([most] + counts)


def ragged(own_key, count, total, reach, slope):
    if count == 2:
        one = jax.random.randint(own_key, (), max(1, total - reach), min(reach, total - 1) + 1)
        return jnp.stack([one, total - one])
    sizes = jnp.asarray(length_profile(count, total, reach, slope), jnp.int32)
    pairs = (count - 1) // 2
    donor, taker = sizes[1:1 + 2 * pairs:2], sizes[2:2 + 2 * pairs:2]
    slack = jnp.minimum(donor - 1, reach - taker)
    moved = jax.random.randint(jax.random.fold_in(own_key, 1), (pairs,), 0, 1 << 20) % (slack + 1)
    sizes = sizes.at[1:1 + 2 * pairs:2].set(donor - moved).at[2:2 + 2 * pairs:2].set(taker + moved)
    return sizes[jax.random.permutation(jax.random.fold_in(own_key, 2), count)]


def centred(stream_key, shape, scale, limit, held_as=jnp.bfloat16):
    values = scale * jax.random.normal(stream_key, shape, jnp.float32)
    return jnp.clip(values, min=-limit, max=limit).astype(held_as)


def setup_inputs(seed: int = 0) -> dict:
    splits = jax.random.split(jax.random.key(seed), 11)
    return {
        "frames": draw_frames(jax.random.fold_in(splits[10], 71), 0),
        "utt_lengths": ragged(splits[1], UTTERANCES, TOKENS, UTT_MOST, 2).astype(jnp.int32),
        "attn_gain": jnp.clip(1.0 + 0.15 * jax.random.normal(splits[2], (D,), jnp.float32), 0.25, 1.75),
        "w_qkv": draw_w_qkv(jax.random.fold_in(splits[10], 71), 0),
        "w_out": centred(splits[4], (D, D), (D // 4) ** -0.5, 0.375),
        "conv_gain": jnp.clip(1.0 + 0.15 * jax.random.normal(splits[5], (D,), jnp.float32), 0.25, 1.75),
        "w_glu": centred(splits[6], (D, 2 * D), D ** -0.5, 0.1875),
        "w_depth": centred(splits[7], (KERNEL, D), KERNEL ** -0.5, 1.0, jnp.float32),
        "depth_gain": jnp.clip(1.0 + 0.15 * jax.random.normal(splits[8], (D,), jnp.float32), 0.25, 1.75),
        "w_proj": centred(splits[9], (D, D), D ** -0.5, 0.1875),
    }


epsilon = 1e-05
big_negative = -1e+30

def normalize(values, row_gain):
    center = values - lax.optimization_barrier(jnp.mean(values, axis=-1, keepdims=True))
    spread = lax.optimization_barrier(jnp.mean(center * center, axis=-1, keepdims=True))
    return center * lax.rsqrt(spread + epsilon) * row_gain

def segment_of(utt_lengths, positions):
    starts = jnp.cumsum(utt_lengths) - utt_lengths
    started = (starts[None, :] <= positions[:, None]).astype(jnp.int32)
    return lax.optimization_barrier(jnp.sum(started, axis=1)) - 1

def one_head(head_qkv, seg_row, score_scale):
    scores = jnp.dot(head_qkv[0], head_qkv[1].T, preferred_element_type=jnp.float32) * score_scale
    allowed = seg_row[:, None] == seg_row[None, :]
    row_max = lax.optimization_barrier(jnp.max(jnp.where(allowed, scores, big_negative), axis=1, keepdims=True))
    weights = jnp.where(allowed, jnp.exp(scores - row_max), 0.0)
    row_total = lax.optimization_barrier(jnp.sum(weights, axis=1, keepdims=True))
    mixed_values = jnp.dot(weights.astype(jnp.bfloat16), head_qkv[2], preferred_element_type=jnp.float32)
    return mixed_values / row_total

def reference(frames, utt_lengths, attn_gain, w_qkv, w_out, conv_gain, w_glu, w_depth, depth_gain, w_proj):
    head_width = D // HEADS
    kernel_half = (KERNEL - 1) // 2
    score_scale = head_width ** (-0.5)
    flat_frames = frames.reshape(TOKENS, D)
    flat_float = flat_frames.astype(jnp.float32)
    frame_seg = segment_of(utt_lengths, jnp.arange(TOKENS, dtype=jnp.int32))
    normed = normalize(flat_float, attn_gain).astype(jnp.bfloat16)
    qkv_rows = jnp.dot(normed, w_qkv, preferred_element_type=jnp.float32).astype(jnp.bfloat16)
    arranged = jnp.transpose(qkv_rows.reshape(GROUPS, WINDOW, HEADS, 3, head_width), (0, 2, 3, 1, 4))
    group_seg = frame_seg.reshape(GROUPS, WINDOW)

    def one_group(operands):
        group_qkv, seg_row = operands
        return lax.map(lambda head_qkv: one_head(head_qkv, seg_row, score_scale), group_qkv)
    heads_out = lax.map(one_group, (arranged, group_seg))
    attended = jnp.transpose(heads_out, (0, 2, 1, 3)).reshape(TOKENS, D).astype(jnp.bfloat16)
    residual = (flat_float + jnp.dot(attended, w_out, preferred_element_type=jnp.float32)).astype(jnp.bfloat16)
    residual = lax.optimization_barrier(residual)
    conv_in = normalize(residual.astype(jnp.float32), conv_gain).astype(jnp.bfloat16)
    projected = jnp.dot(conv_in, w_glu, preferred_element_type=jnp.float32)
    gated = (projected[:, :D] * jax.nn.sigmoid(projected[:, D:])).astype(jnp.bfloat16)
    gated = lax.optimization_barrier(gated)
    padded = jnp.pad(gated.astype(jnp.float32), ((kernel_half, kernel_half), (0, 0)))
    pad_seg = segment_of(utt_lengths, jnp.arange(-kernel_half, TOKENS + kernel_half, dtype=jnp.int32))
    mixed_conv = jnp.zeros((TOKENS, D), jnp.float32)
    for offset in range(KERNEL):
        same_seg = (pad_seg[offset:offset + TOKENS] == frame_seg)[:, None]
        mixed_conv = mixed_conv + jnp.where(same_seg, padded[offset:offset + TOKENS] * w_depth[offset], 0.0)
    normed_conv = normalize(mixed_conv, depth_gain)
    activated = (normed_conv * jax.nn.sigmoid(normed_conv)).astype(jnp.bfloat16)
    result = (residual.astype(jnp.float32) + jnp.dot(activated, w_proj, preferred_element_type=jnp.float32)).astype(jnp.bfloat16)
    return result.reshape(GROUPS, WINDOW, D)
```

```python
import functools

import jax
import jax.numpy as jnp
from jax import lax
from jax.experimental import pallas as pl
from jax.experimental.pallas import tpu as pltpu
from jax.sharding import PartitionSpec as P

HEADS = 16
AXES = ("blk", "grp")
VMEM_BYTES = 56 * 1024 * 1024

epsilon = 1e-05
big_negative = -1e30


def normalize(values, row_gain):
    center = values - jnp.mean(values, axis=-1, keepdims=True)
    spread = jnp.mean(center * center, axis=-1, keepdims=True)
    return center * lax.rsqrt(spread + epsilon) * row_gain


def segment_of(lengths_ref, positions):
    start = jnp.int32(0)
    seg = jnp.full(positions.shape, -1, jnp.int32)
    for c in range(lengths_ref.shape[0]):
        seg = seg + (positions >= start).astype(jnp.int32)
        start = start + lengths_ref[c]
    return seg


def vmem():
    return pl.BlockSpec(memory_space=pltpu.VMEM)


def smem():
    return pl.BlockSpec(memory_space=pltpu.SMEM)


def pack(values):
    half = values.shape[0] // 2
    return jnp.concatenate([values[:half], values[half:]], axis=1)


def unpack(values):
    half = values.shape[1] // 2
    return jnp.concatenate([values[:, :half], values[:, half:]], axis=0)


def qkv_kernel(head_width, frames_ref, gain_ref, *refs):
    weights, out_ref = refs[:-1], refs[-1]
    rows = frames_ref.shape[0]
    normed = normalize(frames_ref[...].astype(jnp.float32), gain_ref[...]).astype(jnp.bfloat16)
    chunk = 0
    for w_ref in weights:
        product = jnp.dot(normed, w_ref[...], preferred_element_type=jnp.float32).astype(
            jnp.bfloat16
        )
        for h in range(w_ref.shape[1] // (3 * head_width)):
            base = 3 * head_width * h
            qk = product[:, base : base + 2 * head_width]
            v = product[:, base + 2 * head_width : base + 3 * head_width]
            out_ref[chunk, :rows, :] = qk
            out_ref[chunk, rows:, :] = pack(v)
            chunk += 1


def attend_kernel(near, stage, stages, head_width, lengths_ref, qkv_ref, out_ref, k_ref, v_ref, s_ref):
    blocks = qkv_ref.shape[0]
    rows = 2 * qkv_ref.shape[1] // 3
    window = blocks * rows
    step = pl.program_id(0)
    group = lax.axis_index("grp")
    place = lax.rem(group // near + stage, stages)
    window_start = (place * near + lax.rem(group, near)) * window

    @pl.when(step == 0)
    def _():
        for b in range(blocks):
            k_ref[b * rows : (b + 1) * rows, :] = qkv_ref[b, :rows, head_width:]
            v = unpack(qkv_ref[b, rows:, :])
            v_ref[b * rows : (b + 1) * rows, :] = jnp.concatenate(
                [v, jnp.ones_like(v)], axis=1
            )

    score_scale = jnp.bfloat16(head_width ** (-0.5))
    queries = qkv_ref[step, :rows, :head_width] * score_scale
    query_seg = segment_of(
        lengths_ref,
        window_start + step * rows + lax.broadcasted_iota(jnp.int32, (rows, 1), 0),
    )
    key_seg = segment_of(
        lengths_ref, window_start + lax.broadcasted_iota(jnp.int32, (1, window), 1)
    )
    row_max = jnp.full((rows, 1), big_negative, jnp.float32)
    for b in range(blocks):
        keys = slice(b * rows, (b + 1) * rows)
        scores = lax.dot_general(
            queries,
            k_ref[keys, :],
            (((1,), (1,)), ((), ())),
            preferred_element_type=jnp.float32,
        )
        scores = jnp.where(query_seg == key_seg[:, keys], scores, big_negative)
        s_ref[:, keys] = scores
        row_max = jnp.maximum(row_max, jnp.max(scores, axis=1, keepdims=True))
    mixed = jnp.zeros((rows, 2 * head_width), jnp.float32)
    for b in range(blocks):
        keys = slice(b * rows, (b + 1) * rows)
        probs = jnp.exp(s_ref[:, keys] - row_max).astype(jnp.bfloat16)
        mixed = mixed + jnp.dot(probs, v_ref[keys, :], preferred_element_type=jnp.float32)
    attended = (mixed[:, :head_width] / mixed[:, head_width:]).astype(jnp.bfloat16)
    out_ref[0] = pack(attended)


def gate_kernel(near, stages, head_width, *refs):
    attended = refs[:stages]
    frames_ref, w_out_ref, gain_ref, w_glu_ref, residual_ref, gated_ref = refs[stages:]
    width = frames_ref.shape[1]
    group = lax.axis_index("grp")
    place, lane = group // near, lax.rem(group, near)
    shard = width // (near * stages)
    total = frames_ref[...].astype(jnp.float32)
    for stage in range(stages):
        base = lax.rem(place + stages - stage, stages) * near
        count = attended[stage].shape[0] // near
        for o in range(near):
            row0 = pl.multiple_of((base + lax.rem(lane + o, near)) * shard, shard)
            pieces = [unpack(attended[stage][o * count + i]) for i in range(count)]
            left = jnp.concatenate(pieces, axis=1)
            total = total + jnp.dot(
                left, w_out_ref[pl.ds(row0, shard), :], preferred_element_type=jnp.float32
            )
    residual = total.astype(jnp.bfloat16)
    residual_ref[...] = residual
    conv_in = normalize(residual.astype(jnp.float32), gain_ref[...]).astype(jnp.bfloat16)
    tile = min(256, width)
    for c in range(0, width, tile):
        a = jnp.dot(conv_in, w_glu_ref[:, c : c + tile], preferred_element_type=jnp.float32)
        gate = jnp.dot(
            conv_in, w_glu_ref[:, width + c : width + c + tile], preferred_element_type=jnp.float32
        )
        gated_ref[:, c : c + tile] = (a * jax.nn.sigmoid(gate)).astype(jnp.bfloat16)


def conv_kernel(
    blocks, taps, lengths_ref, low_ref, gated_ref, high_ref, residual_ref, w_depth_ref, gain_ref,
    w_proj_ref, out_ref, ext_ref, mixed_ref,
):
    rows, width = gated_ref.shape
    halo = low_ref.shape[0]
    half = (taps - 1) // 2
    first = (lax.axis_index("grp") * blocks + lax.axis_index("blk")) * rows
    ext_ref[:halo, :] = low_ref[...].astype(jnp.float32)
    ext_ref[halo : halo + rows, :] = gated_ref[...].astype(jnp.float32)
    ext_ref[halo + rows :, :] = high_ref[...].astype(jnp.float32)
    tall, wide = 32, 256

    for r in range(0, rows, tall):
        start = first + r
        edges = jnp.int32(0)
        edge = jnp.int32(0)
        for c in range(lengths_ref.shape[0] - 1):
            edge = edge + lengths_ref[c]
            inside = jnp.logical_and(edge > start - half, edge < start + tall + half)
            edges = edges + inside.astype(jnp.int32)
        source = r + halo - half

        @pl.when(edges == 0)
        def _(r=r, source=source):
            for c in range(0, width, wide):
                cols = slice(c, c + wide)
                mixed = jnp.zeros((tall, wide), jnp.float32)
                for t in range(taps):
                    values = ext_ref[source + t : source + t + tall, cols]
                    mixed = mixed + values * w_depth_ref[t : t + 1, cols]
                mixed_ref[r : r + tall, cols] = mixed

        @pl.when(edges > 0)
        def _(r=r, source=source, start=start):
            column = lax.broadcasted_iota(jnp.int32, (tall, 128), 0)
            own = segment_of(lengths_ref, start + column)
            for c in range(0, width, 128):
                cols = slice(c, c + 128)
                mixed = jnp.zeros((tall, 128), jnp.float32)
                for t in range(taps):
                    same = segment_of(lengths_ref, start + t - half + column) == own
                    values = ext_ref[source + t : source + t + tall, cols]
                    mixed = mixed + jnp.where(same, values * w_depth_ref[t : t + 1, cols], 0.0)
                mixed_ref[r : r + tall, cols] = mixed

    normed = normalize(mixed_ref[...], gain_ref[...])
    activated = (normed * jax.nn.sigmoid(normed)).astype(jnp.bfloat16)
    out_ref[...] = (
        residual_ref[...].astype(jnp.float32)
        + jnp.dot(activated, w_proj_ref[...], preferred_element_type=jnp.float32)
    ).astype(jnp.bfloat16)


def params():
    return pltpu.CompilerParams(vmem_limit_bytes=VMEM_BYTES)


def body(
    sizes, frames, utt_lengths, attn_gain, w_qkv, w_out, conv_gain, w_glu, w_depth, depth_gain, w_proj
):
    blocks, groups = sizes
    rows, width = frames.shape[1:]
    head_width = width // HEADS
    stages = HEADS // blocks
    near = groups // stages
    taps = w_depth.shape[0]
    window = rows * blocks
    bf16 = jnp.bfloat16
    local = frames[0]

    def index(b, g):
        return b * groups + g

    def moved(value, target):
        pairs = []
        for b in range(blocks):
            for g in range(groups):
                to = target(b, g)
                if to is not None:
                    pairs.append((index(b, g), index(*to)))
        return lax.ppermute(value, AXES, pairs)

    def shifted(p, c, by):
        return ((p + by) % stages) * near + c

    if stages == 1:
        whole = lax.all_gather(w_qkv, "grp", axis=0)
        lane = lax.axis_index("grp")
        weights = [
            lax.dynamic_index_in_dim(whole, (lane + o) % near, 0, keepdims=False) for o in range(near)
        ]
    else:
        weights = [w_qkv] + [
            moved(w_qkv, lambda b, g, o=o: (b, g // near * near + (g - o) % near))
            for o in range(1, near)
        ]
    sources = [local] + [
        moved(local, lambda b, g, t=t: (b, shifted(g // near, g % near, -t)))
        for t in range(1, stages)
    ]
    chunk = 3 * rows // 2
    gain_row = attn_gain[None]
    returned = []
    for t in range(stages):
        packed = pl.pallas_call(
            functools.partial(qkv_kernel, head_width),
            out_shape=jax.ShapeDtypeStruct((blocks, chunk, 2 * head_width), bf16),
            in_specs=[vmem()] * (2 + near),
            out_specs=vmem(),
            compiler_params=params(),
            name=f"qkv_{t}",
        )(sources[t], gain_row, *weights)
        mine = lax.all_to_all(packed, "blk", split_axis=0, concat_axis=0, tiled=True)
        attended = pl.pallas_call(
            functools.partial(attend_kernel, near, t, stages, head_width),
            out_shape=jax.ShapeDtypeStruct((blocks, rows // 2, 2 * head_width), bf16),
            grid=(blocks,),
            in_specs=[
                smem(),
                pl.BlockSpec((blocks, chunk, 2 * head_width), lambda i: (0, 0, 0)),
            ],
            out_specs=pl.BlockSpec((1, rows // 2, 2 * head_width), lambda i: (i, 0, 0)),
            scratch_shapes=[
                pltpu.VMEM((window, head_width), bf16),
                pltpu.VMEM((window, 2 * head_width), bf16),
                pltpu.VMEM((rows, window), jnp.float32),
            ],
            compiler_params=params(),
            name=f"attend_{t}",
        )(utt_lengths, mine)
        back = lax.all_to_all(attended, "blk", split_axis=0, concat_axis=0, tiled=True)
        if t:
            back = moved(back, lambda b, g, t=t: (b, shifted(g // near, g % near, t)))
        returned.append(back)

    residual, gated = pl.pallas_call(
        functools.partial(gate_kernel, near, stages, head_width),
        out_shape=[jax.ShapeDtypeStruct((rows, width), bf16)] * 2,
        in_specs=[vmem()] * (stages + 4),
        out_specs=[vmem()] * 2,
        compiler_params=params(),
        name="gate",
    )(*returned, local, w_out, conv_gain[None], w_glu)

    def neighbour(by):
        def target(b, g):
            place = g * blocks + b + by
            if 0 <= place < blocks * groups:
                return (place % blocks, place // blocks)
            return None

        return target

    halo = 16 * pl.cdiv((taps - 1) // 2, 16)
    low = moved(gated[rows - halo :], neighbour(1))
    high = moved(gated[:halo], neighbour(-1))
    result = pl.pallas_call(
        functools.partial(conv_kernel, blocks, taps),
        out_shape=jax.ShapeDtypeStruct((rows, width), bf16),
        in_specs=[smem()] + [vmem()] * 7,
        out_specs=vmem(),
        scratch_shapes=[
            pltpu.VMEM((rows + 2 * halo, width), jnp.float32),
            pltpu.VMEM((rows, width), jnp.float32),
        ],
        compiler_params=params(),
        name="conv",
    )(utt_lengths, low, gated, high, residual, w_depth, depth_gain[None], w_proj)
    return result[None]


def solution(mesh):
    in_specs = (P("grp", "blk", None), P(), P(), P(None, "grp"), P(), P(), P(), P(), P(), P())
    out_specs = P("grp", "blk", None)
    sizes = (mesh.shape["blk"], mesh.shape["grp"])
    return jax.shard_map(
        functools.partial(body, sizes),
        mesh=mesh,
        in_specs=in_specs,
        out_specs=out_specs,
        check_vma=False,
    )
```
